32 devices in a mesh: vocab: 8 (over y, x, core), hid: 4 (over z).
Axes of the slice: x: 2, y: 2, z: 4, core: 2. Of those that a mesh axis runs over, the one named last changes fastest.
Arguments:
- hidden: bfloat16 [2, 256, 7168], P(None, 'vocab', 'hid'), may hold values from -100 to 100
- head_weight: bfloat16 [7168, 65536], P('hid', 'vocab'), may hold values from -2 to 2
- targets: int32 [2, 256], P(None, 'hid'), may hold values from 0 to 65535
Outputs:
- entropy: float32 [2, 256], P(None, 'hid')
- squared: float32 [2, 256], P(None, 'hid')
The draws below stay inside these ranges and needn't reach their ends.
All inputs are finite; a program needn't handle non-finite values.
Results may differ from the reference program's by a relative error of at most 0.0003.
Values may be sent and summed in bfloat16 or wider, within the bound.
A program may use at most 192 MiB of HBM per device.

```python
import math
import jax
import jax.numpy as jnp

D = 7168
DEPTH = 2
VOCAB = 65536
TOKENS = 256


def column_block(key, index):
    block_key = jax.random.fold_in(jax.random.fold_in(key, 7001), index)
    column_ids = index * 128 + jnp.arange(128)
    column_ramp = 1.0 + 0.25 * column_ids.astype(jnp.float32) / VOCAB
    raw_values = jnp.clip(jax.random.normal(block_key, (D, 128), jnp.float32), -6.0, 6.0)
    return raw_values * column_ramp[None, :] / math.sqrt(D)


def draw_head_weight(key, part):
    blocks = jax.vmap(lambda index: column_block(key, index))(jnp.arange(VOCAB // 128))
    return jnp.transpose(blocks, (1, 0, 2)).reshape(D, VOCAB).astype(jnp.bfloat16)


def draw_hidden(key, part):
    hidden_key = jax.random.fold_in(key, 7002)
    base_values = 3.0 * jnp.clip(jax.random.normal(hidden_key, (DEPTH, TOKENS, D), jnp.float32), -6.0, 6.0)
    return jnp.clip(base_values, -100.0, 100.0).astype(jnp.bfloat16)


def touch_ends(result, rng, smallest, high):
    longest = result.shape.index(max(result.shape))
    spots = []
    for shift in (0, 1):
        where = [jax.random.randint(jax.random.fold_in(rng, axis), (), 0, length) for axis, length in enumerate(result.shape)]
        where[longest] = (where[longest] + shift) % result.shape[longest]
        spots.append(tuple(where))
    return result.at[spots[0]].set(smallest).at[spots[1]].set(high)


def setup_inputs(seed: int = 0) -> dict:
    key_of = jax.random.split(jax.random.key(seed), 4)
    hidden = draw_hidden(jax.random.fold_in(key_of[3], 71), 0)
    head_weight = draw_head_weight(jax.random.fold_in(key_of[3], 71), 0)
    targets = touch_ends(jax.random.randint(key_of[2], (DEPTH, TOKENS), 0, VOCAB), jax.random.fold_in(key_of[2], 1), 0, VOCAB - 1).astype(jnp.int32)
    return dict(hidden=hidden, head_weight=head_weight, targets=targets)


def reference(hidden, head_weight, targets):
    entropy_rows = []
    square_rows = []
    for depth_index in range(DEPTH):
        logits = jnp.dot(hidden[depth_index], head_weight, preferred_element_type=jnp.float32)
        row_peak = jnp.max(logits, axis=1)
        row_total = jnp.sum(jnp.exp(logits - row_peak[:, None]), axis=1)
        log_norm = row_peak + jnp.log(row_total)
        picked = jnp.take_along_axis(logits, targets[depth_index][:, None], axis=1)[:, 0]
        entropy_rows.append(log_norm - picked)
        square_rows.append(log_norm * log_norm)
    return jnp.stack(entropy_rows), jnp.stack(square_rows)
```

```python
import functools

import jax
import jax.numpy as jnp
from jax import lax
from jax.experimental import pallas as pl
from jax.experimental.pallas import tpu as pltpu
from jax.sharding import PartitionSpec as P

MESH = pl.DeviceIdType.MESH
LANES = 128
SKEW = 2
LOWEST = -3.0e38
TOP = 32767.0


def kernel(
    n, nv, nj, cw,
    hidden, weight, targets,
    entropy, squared,
    rows, wbuf, came, gone, came_scale, gone_scale, part,
    labels, label_tile, peak, mass, pick, ends, mine, shared,
    w_sem, own_sem, h_send, h_recv, l_send, l_recv,
    q_send, q_recv, s_send, s_recv, e_send, e_recv, c_send, c_recv,
):
    v, me = lax.axis_index("vocab"), lax.axis_index("hid")
    groups = nv // 2
    chip, parity = v // 2, v % 2
    share = hidden.shape[1]
    block = rows.shape[1] * rows.shape[2]
    total = groups * nj
    half = nj * cw
    chains = ((me, me + 1), (n - 1 - me, me - 1))

    def w_copy(way, j):
        return pltpu.make_async_copy(
            weight.at[:, pl.ds(way * half + pl.multiple_of(j * cw, cw), cw)],
            wbuf.at[way * nj + j],
            w_sem.at[way * nj + j],
        )

    def place(b):
        return rows.at[b // 2, :, pl.ds(pl.multiple_of((b % 2) * share, share), share), :]

    own = pltpu.make_async_copy(hidden, place(v), own_sem)
    own.start()
    for j in range(2):
        for way in range(2):
            w_copy(way, j).start()

    barrier = pltpu.get_barrier_semaphore()
    for k in range(1, nv):
        pl.semaphore_signal(barrier, inc=1, device_id=((v + k) % nv, me), device_id_type=MESH)
    for k in range(1, n):
        pl.semaphore_signal(barrier, inc=1, device_id=(v, (me + k) % n), device_id_type=MESH)
    pl.semaphore_wait(barrier, nv - 1 + n - 1)

    def h_copy(slot, target):
        return pltpu.make_async_remote_copy(
            src_ref=hidden, dst_ref=place(v), send_sem=h_send.at[slot], recv_sem=h_recv.at[v],
            device_id=(target, me), device_id_type=MESH,
        )

    def h_arrival(b):
        return pltpu.make_async_remote_copy(
            src_ref=hidden, dst_ref=place(b), send_sem=h_send.at[0], recv_sem=h_recv.at[b],
            device_id=(v, me), device_id_type=MESH,
        )

    peers = [2 * chip + 1 - parity]
    for back in range(1, groups):
        other = (chip - back + groups) % groups
        peers += [2 * other + parity, 2 * other + 1 - parity]
    h_copies = [h_copy(slot, target) for slot, target in enumerate(peers)]
    for copy in h_copies:
        copy.start()

    finals = (n - 1, 0)

    def l_copy(e):
        return pltpu.make_async_remote_copy(
            src_ref=targets, dst_ref=labels.at[me], send_sem=l_send.at[e], recv_sem=l_recv.at[me],
            device_id=(v, finals[e]), device_id_type=MESH,
        )

    for e in range(2):
        @pl.when(me != finals[e])
        def _():
            l_copy(e).start()

        @pl.when(me == finals[e])
        def _():
            labels[me] = targets[...]

    is_end = jnp.logical_or(me == 0, me == n - 1)

    def message(way, k, target):
        data = pltpu.make_async_remote_copy(
            src_ref=gone.at[way, k], dst_ref=came.at[way, k],
            send_sem=q_send.at[way, k], recv_sem=q_recv.at[way, k],
            device_id=(v, target), device_id_type=MESH,
        )
        scale = pltpu.make_async_remote_copy(
            src_ref=gone_scale.at[way, k], dst_ref=came_scale.at[way, k],
            send_sem=s_send.at[way, k], recv_sem=s_recv.at[way, k],
            device_id=(v, target), device_id_type=MESH,
        )
        return data, scale

    def send_end(e, g):
        return pltpu.make_async_remote_copy(
            src_ref=ends.at[g], dst_ref=mine.at[e], send_sem=e_send.at[g], recv_sem=e_recv.at[e],
            device_id=(v, g), device_id_type=MESH,
        )

    def statistics(way, g, j):
        @pl.when(j == 0)
        def _():
            line = labels[g]
            line = jnp.concatenate([line[0:1, :], line[1:2, :]], axis=1)
            label_tile[...] = jnp.transpose(jnp.broadcast_to(line, (block, block)))
            peak[...] = jnp.full_like(peak, LOWEST)
            mass[...] = jnp.zeros_like(mass)
            pick[...] = jnp.zeros_like(pick)

        x = part[way]
        pieces = [x[:, c * LANES : (c + 1) * LANES] for c in range(cw // LANES)]
        old = peak[...]
        new = functools.reduce(jnp.maximum, pieces, old)
        peak[...] = new
        mass[...] = mass[...] * jnp.exp(old - new) + sum(jnp.exp(piece - new) for piece in pieces)
        first = v * (2 * half) + way * half + j * cw
        offset = label_tile[...] - first
        lane = lax.broadcasted_iota(jnp.int32, (block, LANES), 1)
        found = pick[...]
        for c, piece in enumerate(pieces):
            found = found + jnp.where(offset == lane + c * LANES, piece, 0.0)
        pick[...] = found

        @pl.when(j == nj - 1)
        def _():
            tall = jnp.transpose(peak[...])
            top = jnp.max(tall, axis=0, keepdims=True)
            weight_sum = jnp.sum(jnp.transpose(mass[...]) * jnp.exp(tall - top), axis=0, keepdims=True)
            chosen = jnp.sum(jnp.transpose(pick[...]), axis=0, keepdims=True)
            ends[g] = jnp.concatenate([top, weight_sum, chosen, jnp.zeros((5, block), jnp.float32)], axis=0)

            @pl.when(g != me)
            def _():
                send_end(way, g).start()

            @pl.when(g == me)
            def _():
                mine[way] = ends[g]

    def process(way, k):
        pos, target = chains[way]
        rb, j = k // nj, k % nj
        g = (chip + rb) % groups

        @pl.when(rb == 0)
        def _():
            @pl.when(j + 2 < nj)
            def _():
                w_copy(way, j + 2).start()

            w_copy(way, j).wait()

        a = rows[g].reshape(block, rows.shape[3])
        part[way] = jnp.dot(a, wbuf[way * nj + j], preferred_element_type=jnp.float32)

        @pl.when(pos > 0)
        def _():
            for copy in message(way, k, me):
                copy.wait_recv()
            part[way] += came[way, k].astype(jnp.int32).astype(jnp.float32) * came_scale[way, k]

        @pl.when(pos < n - 1)
        def _():
            x = part[way]
            largest = jnp.maximum(jnp.max(jnp.abs(x), axis=0, keepdims=True), 1e-30)
            gone_scale[way, k] = largest * (1.0 / TOP)
            gone[way, k] = jnp.round(x * (TOP / largest)).astype(jnp.int32).astype(jnp.int16)
            for copy in message(way, k, target):
                copy.start()

        @pl.when(pos == n - 1)
        def _():
            statistics(way, g, j)

    nearest = jnp.minimum(me, n - 1 - me)
    own.wait()

    @pl.when(is_end)
    def _():
        for z in range(n):
            @pl.when(me != z)
            def _():
                pltpu.make_async_remote_copy(
                    src_ref=targets, dst_ref=labels.at[z], send_sem=l_send.at[0], recv_sem=l_recv.at[z],
                    device_id=(v, me), device_id_type=MESH,
                ).wait_recv()

    def step(i, carry):
        lead = i - nearest * SKEW

        @pl.when(jnp.logical_and(lead >= 0, jnp.logical_and(lead < total, lead % nj == 0)))
        def _():
            rb = lead // nj
            g = (chip + rb) % groups
            for side in range(2):
                @pl.when(2 * g + side != v)
                def _():
                    h_arrival(2 * g + side).wait_recv()

        for way in range(2):
            k = i - chains[way][0] * SKEW

            @pl.when(jnp.logical_and(k >= 0, k < total))
            def _():
                process(way, k)

        return carry

    lax.fori_loop(0, total + (n - 1) * SKEW, step, 0)

    for e in range(2):
        @pl.when(me != finals[e])
        def _():
            send_end(e, me).wait_recv()

    def merge(tiles):
        top = functools.reduce(jnp.maximum, [t[0:1] for t in tiles])
        weight_sum = sum(t[1:2] * jnp.exp(t[0:1] - top) for t in tiles)
        chosen = sum(t[2:3] for t in tiles)
        return top, weight_sum, chosen

    top, weight_sum, chosen = merge([mine[0], mine[1]])
    shared[v] = jnp.concatenate([top, weight_sum, chosen, jnp.zeros((5, block), jnp.float32)], axis=0)

    def c_copy(slot, source, target):
        return pltpu.make_async_remote_copy(
            src_ref=shared.at[source], dst_ref=shared.at[source], send_sem=c_send.at[slot], recv_sem=c_recv.at[source],
            device_id=(target, me), device_id_type=MESH,
        )

    for k in range(1, nv):
        c_copy(k - 1, v, (v + k) % nv).start()
    for k in range(1, nv):
        c_copy(0, (v + k) % nv, v).wait_recv()
    top, weight_sum, chosen = merge([shared[k] for k in range(nv)])
    norm = top + jnp.log(weight_sum)
    loss, square = norm - chosen, norm * norm
    width = block // 2
    for a in range(2):
        entropy[a : a + 1, :] = loss[:, a * width : (a + 1) * width]
        squared[a : a + 1, :] = square[:, a * width : (a + 1) * width]

    for copy in h_copies:
        copy.wait_send()
    for e in range(2):
        @pl.when(me != finals[e])
        def _():
            l_copy(e).wait_send()
    for way in range(2):
        pos, target = chains[way]

        @pl.when(pos < n - 1)
        def _():
            def drain(k, carry):
                for copy in message(way, k, target):
                    copy.wait_send()
                return carry

            lax.fori_loop(0, total, drain, 0)

        @pl.when(pos == n - 1)
        def _():
            for g in range(groups):
                @pl.when(me != g)
                def _():
                    send_end(way, g).wait_send()
    for k in range(1, nv):
        c_copy(k - 1, v, (v + k) % nv).wait_send()


def body(n, nv, hidden, head_weight, targets):
    depths, share, width = hidden.shape
    columns = head_weight.shape[1]
    groups = nv // 2
    assert groups == n and depths == 2 and depths * 2 * share == LANES
    cw = min(512, columns // 2)
    nj = columns // 2 // cw
    total = groups * nj
    block = depths * 2 * share
    vmem, anywhere = pl.BlockSpec(memory_space=pltpu.VMEM), pl.BlockSpec(memory_space=pl.ANY)
    dma = pltpu.SemaphoreType.DMA
    return pl.pallas_call(
        functools.partial(kernel, n, nv, nj, cw),
        out_shape=[jax.ShapeDtypeStruct(targets.shape, jnp.float32)] * 2,
        in_specs=[anywhere, anywhere, vmem],
        out_specs=[vmem, vmem],
        scratch_shapes=[
            pltpu.VMEM((groups, depths, 2 * share, width), hidden.dtype),
            pltpu.VMEM((2 * nj, width, cw), head_weight.dtype),
            pltpu.VMEM((2, total, block, cw), jnp.int16),
            pltpu.VMEM((2, total, block, cw), jnp.int16),
            pltpu.VMEM((2, total, 1, cw), jnp.float32),
            pltpu.VMEM((2, total, 1, cw), jnp.float32),
            pltpu.VMEM((2, block, cw), jnp.float32),
            pltpu.VMEM((n,) + targets.shape, jnp.int32),
            pltpu.VMEM((block, LANES), jnp.int32),
            pltpu.VMEM((block, LANES), jnp.float32),
            pltpu.VMEM((block, LANES), jnp.float32),
            pltpu.VMEM((block, LANES), jnp.float32),
            pltpu.VMEM((groups, 8, block), jnp.float32),
            pltpu.VMEM((2, 8, block), jnp.float32),
            pltpu.VMEM((nv, 8, block), jnp.float32),
            dma((2 * nj,)), dma, dma((nv - 1,)), dma((nv,)), dma((2,)), dma((n,)),
            dma((2, total)), dma((2, total)), dma((2, total)), dma((2, total)),
            dma((groups,)), dma((2,)), dma((nv - 1,)), dma((nv,)),
        ],
        compiler_params=pltpu.CompilerParams(
            collective_id=0, has_side_effects=True, vmem_limit_bytes=60 * 1024 * 1024
        ),
    )(hidden, head_weight, targets)


def solution(mesh):
    return jax.shard_map(
        functools.partial(body, mesh.shape["hid"], mesh.shape["vocab"]),
        mesh=mesh,
        in_specs=(P(None, "vocab", "hid"), P("hid", "vocab"), P(None, "hid")),
        out_specs=(P(None, "hid"), P(None, "hid")),
        check_vma=False,
    )
```

```python
import functools

import jax
import jax.numpy as jnp
from jax import lax
from jax.experimental import pallas as pl
from jax.experimental.pallas import tpu as pltpu
from jax.sharding import PartitionSpec as P

MESH = pl.DeviceIdType.MESH
LANES = 128
SKEW = 4
LOWEST = -3.0e38
TOP = 32767.0


def kernel(
    n, nv, nj, cw,
    hidden, weight, targets,
    entropy, squared,
    rows, wbuf, came, gone, came_scale, gone_scale, part,
    labels, label_tile, peak, mass, pick, ends, mine, shared,
    w_sem, own_sem, h_send, h_recv, l_send, l_recv,
    q_send, q_recv, s_send, s_recv, e_send, e_recv, c_send, c_recv,
):
    v, me = lax.axis_index("vocab"), lax.axis_index("hid")
    groups = nv // 2
    chip, parity = v // 2, v % 2
    share = hidden.shape[1]
    block = rows.shape[1] * rows.shape[2]
    total = groups * nj
    half = nj * cw
    chains = ((me, me + 1), (n - 1 - me, me - 1))

    def w_copy(way, j):
        return pltpu.make_async_copy(
            weight.at[:, pl.ds(way * half + pl.multiple_of(j * cw, cw), cw)],
            wbuf.at[way * nj + j],
            w_sem.at[way * nj + j],
        )

    def place(b):
        return rows.at[b // 2, :, pl.ds(pl.multiple_of((b % 2) * share, share), share), :]

    own = pltpu.make_async_copy(hidden, place(v), own_sem)
    own.start()
    for j in range(2):
        for way in range(2):
            w_copy(way, j).start()

    barrier = pltpu.get_barrier_semaphore()
    for k in range(1, nv):
        pl.semaphore_signal(barrier, inc=1, device_id=((v + k) % nv, me), device_id_type=MESH)
    for k in range(1, n):
        pl.semaphore_signal(barrier, inc=1, device_id=(v, (me + k) % n), device_id_type=MESH)
    pl.semaphore_wait(barrier, nv - 1 + n - 1)

    def h_copy(slot, target):
        return pltpu.make_async_remote_copy(
            src_ref=hidden, dst_ref=place(v), send_sem=h_send.at[slot], recv_sem=h_recv.at[v],
            device_id=(target, me), device_id_type=MESH,
        )

    def h_arrival(b):
        return pltpu.make_async_remote_copy(
            src_ref=hidden, dst_ref=place(b), send_sem=h_send.at[0], recv_sem=h_recv.at[b],
            device_id=(v, me), device_id_type=MESH,
        )

    peers = [2 * chip + 1 - parity]
    for back in range(1, groups):
        other = (chip - back + groups) % groups
        peers += [2 * other + parity, 2 * other + 1 - parity]
    h_copies = [h_copy(slot, target) for slot, target in enumerate(peers)]
    for copy in h_copies:
        copy.start()

    finals = (n - 1, 0)

    def l_copy(e):
        return pltpu.make_async_remote_copy(
            src_ref=targets, dst_ref=labels.at[me], send_sem=l_send.at[e], recv_sem=l_recv.at[me],
            device_id=(v, finals[e]), device_id_type=MESH,
        )

    for e in range(2):
        @pl.when(me != finals[e])
        def _():
            l_copy(e).start()

        @pl.when(me == finals[e])
        def _():
            labels[me] = targets[...]

    is_end = jnp.logical_or(me == 0, me == n - 1)

    def message(way, k, target):
        data = pltpu.make_async_remote_copy(
            src_ref=gone.at[way, k], dst_ref=came.at[way, k],
            send_sem=q_send.at[way, k], recv_sem=q_recv.at[way, k],
            device_id=(v, target), device_id_type=MESH,
        )
        scale = pltpu.make_async_remote_copy(
            src_ref=gone_scale.at[way, k], dst_ref=came_scale.at[way, k],
            send_sem=s_send.at[way, k], recv_sem=s_recv.at[way, k],
            device_id=(v, target), device_id_type=MESH,
        )
        return data, scale

    def send_end(e, g):
        return pltpu.make_async_remote_copy(
            src_ref=ends.at[g], dst_ref=mine.at[e], send_sem=e_send.at[g], recv_sem=e_recv.at[e],
            device_id=(v, g), device_id_type=MESH,
        )

    def statistics(way, g, j):
        @pl.when(j == 0)
        def _():
            line = labels[g]
            line = jnp.concatenate([line[0:1, :], line[1:2, :]], axis=1)
            label_tile[...] = jnp.transpose(jnp.broadcast_to(line, (block, block)))
            peak[...] = jnp.full_like(peak, LOWEST)
            mass[...] = jnp.zeros_like(mass)
            pick[...] = jnp.zeros_like(pick)

        x = part[way]
        pieces = [x[:, c * LANES : (c + 1) * LANES] for c in range(cw // LANES)]
        old = peak[...]
        new = functools.reduce(jnp.maximum, pieces, old)
        peak[...] = new
        mass[...] = mass[...] * jnp.exp(old - new) + sum(jnp.exp(piece - new) for piece in pieces)
        first = v * (2 * half) + way * half + j * cw
        offset = label_tile[...] - first
        lane = lax.broadcasted_iota(jnp.int32, (block, LANES), 1)
        found = pick[...]
        for c, piece in enumerate(pieces):
            found = found + jnp.where(offset == lane + c * LANES, piece, 0.0)
        pick[...] = found

        @pl.when(j == nj - 1)
        def _():
            tall = jnp.transpose(peak[...])
            top = jnp.max(tall, axis=0, keepdims=True)
            weight_sum = jnp.sum(jnp.transpose(mass[...]) * jnp.exp(tall - top), axis=0, keepdims=True)
            chosen = jnp.sum(jnp.transpose(pick[...]), axis=0, keepdims=True)
            ends[g] = jnp.concatenate([top, weight_sum, chosen, jnp.zeros((5, block), jnp.float32)], axis=0)

            @pl.when(g != me)
            def _():
                send_end(way, g).start()

            @pl.when(g == me)
            def _():
                mine[way] = ends[g]

    def process(way, k):
        pos, target = chains[way]
        rb, j = k // nj, k % nj
        g = (chip + rb) % groups

        @pl.when(rb == 0)
        def _():
            @pl.when(j + 2 < nj)
            def _():
                w_copy(way, j + 2).start()

            w_copy(way, j).wait()

        a = rows[g].reshape(block, rows.shape[3])
        part[way] = jnp.dot(a, wbuf[way * nj + j], preferred_element_type=jnp.float32)

        @pl.when(pos > 0)
        def _():
            for copy in message(way, k, me):
                copy.wait_recv()
            part[way] += came[way, k].astype(jnp.int32).astype(jnp.float32) * came_scale[way, k]

        @pl.when(pos < n - 1)
        def _():
            x = part[way]
            largest = jnp.maximum(jnp.max(jnp.abs(x), axis=0, keepdims=True), 1e-30)
            gone_scale[way, k] = largest * (1.0 / TOP)
            gone[way, k] = jnp.round(x * (TOP / largest)).astype(jnp.int32).astype(jnp.int16)
            for copy in message(way, k, target):
                copy.start()

        @pl.when(pos == n - 1)
        def _():
            statistics(way, g, j)

    nearest = jnp.minimum(me, n - 1 - me)
    own.wait()

    @pl.when(is_end)
    def _():
        for z in range(n):
            @pl.when(me != z)
            def _():
                pltpu.make_async_remote_copy(
                    src_ref=targets, dst_ref=labels.at[z], send_sem=l_send.at[0], recv_sem=l_recv.at[z],
                    device_id=(v, me), device_id_type=MESH,
                ).wait_recv()

    def step(i, carry):
        lead = i - nearest * SKEW

        @pl.when(jnp.logical_and(lead >= 0, jnp.logical_and(lead < total, lead % nj == 0)))
        def _():
            rb = lead // nj
            g = (chip + rb) % groups
            for side in range(2):
                @pl.when(2 * g + side != v)
                def _():
                    h_arrival(2 * g + side).wait_recv()

        for way in range(2):
            k = i - chains[way][0] * SKEW

            @pl.when(jnp.logical_and(k >= 0, k < total))
            def _():
                process(way, k)

        return carry

    lax.fori_loop(0, total + (n - 1) * SKEW, step, 0)

    for e in range(2):
        @pl.when(me != finals[e])
        def _():
            send_end(e, me).wait_recv()

    def merge(tiles):
        top = functools.reduce(jnp.maximum, [t[0:1] for t in tiles])
        weight_sum = sum(t[1:2] * jnp.exp(t[0:1] - top) for t in tiles)
        chosen = sum(t[2:3] for t in tiles)
        return top, weight_sum, chosen

    top, weight_sum, chosen = merge([mine[0], mine[1]])
    shared[v] = jnp.concatenate([top, weight_sum, chosen, jnp.zeros((5, block), jnp.float32)], axis=0)

    def c_copy(slot, source, target):
        return pltpu.make_async_remote_copy(
            src_ref=shared.at[source], dst_ref=shared.at[source], send_sem=c_send.at[slot], recv_sem=c_recv.at[source],
            device_id=(target, me), device_id_type=MESH,
        )

    for k in range(1, nv):
        c_copy(k - 1, v, (v + k) % nv).start()
    for k in range(1, nv):
        c_copy(0, (v + k) % nv, v).wait_recv()
    top, weight_sum, chosen = merge([shared[k] for k in range(nv)])
    norm = top + jnp.log(weight_sum)
    loss, square = norm - chosen, norm * norm
    width = block // 2
    for a in range(2):
        entropy[a : a + 1, :] = loss[:, a * width : (a + 1) * width]
        squared[a : a + 1, :] = square[:, a * width : (a + 1) * width]

    for copy in h_copies:
        copy.wait_send()
    for e in range(2):
        @pl.when(me != finals[e])
        def _():
            l_copy(e).wait_send()
    for way in range(2):
        pos, target = chains[way]

        @pl.when(pos < n - 1)
        def _():
            def drain(k, carry):
                for copy in message(way, k, target):
                    copy.wait_send()
                return carry

            lax.fori_loop(0, total, drain, 0)

        @pl.when(pos == n - 1)
        def _():
            for g in range(groups):
                @pl.when(me != g)
                def _():
                    send_end(way, g).wait_send()
    for k in range(1, nv):
        c_copy(k - 1, v, (v + k) % nv).wait_send()


def body(n, nv, hidden, head_weight, targets):
    depths, share, width = hidden.shape
    columns = head_weight.shape[1]
    groups = nv // 2
    assert groups == n and depths == 2 and depths * 2 * share == LANES
    cw = min(256, columns // 2)
    nj = columns // 2 // cw
    total = groups * nj
    block = depths * 2 * share
    vmem, anywhere = pl.BlockSpec(memory_space=pltpu.VMEM), pl.BlockSpec(memory_space=pl.ANY)
    dma = pltpu.SemaphoreType.DMA
    return pl.pallas_call(
        functools.partial(kernel, n, nv, nj, cw),
        out_shape=[jax.ShapeDtypeStruct(targets.shape, jnp.float32)] * 2,
        in_specs=[anywhere, anywhere, vmem],
        out_specs=[vmem, vmem],
        scratch_shapes=[
            pltpu.VMEM((groups, depths, 2 * share, width), hidden.dtype),
            pltpu.VMEM((2 * nj, width, cw), head_weight.dtype),
            pltpu.VMEM((2, total, block, cw), jnp.int16),
            pltpu.VMEM((2, total, block, cw), jnp.int16),
            pltpu.VMEM((2, total, 1, cw), jnp.float32),
            pltpu.VMEM((2, total, 1, cw), jnp.float32),
            pltpu.VMEM((2, block, cw), jnp.float32),
            pltpu.VMEM((n,) + targets.shape, jnp.int32),
            pltpu.VMEM((block, LANES), jnp.int32),
            pltpu.VMEM((block, LANES), jnp.float32),
            pltpu.VMEM((block, LANES), jnp.float32),
            pltpu.VMEM((block, LANES), jnp.float32),
            pltpu.VMEM((groups, 8, block), jnp.float32),
            pltpu.VMEM((2, 8, block), jnp.float32),
            pltpu.VMEM((nv, 8, block), jnp.float32),
            dma((2 * nj,)), dma, dma((nv - 1,)), dma((nv,)), dma((2,)), dma((n,)),
            dma((2, total)), dma((2, total)), dma((2, total)), dma((2, total)),
            dma((groups,)), dma((2,)), dma((nv - 1,)), dma((nv,)),
        ],
        compiler_params=pltpu.CompilerParams(
            collective_id=0, has_side_effects=True, vmem_limit_bytes=60 * 1024 * 1024
        ),
    )(hidden, head_weight, targets)


def solution(mesh):
    return jax.shard_map(
        functools.partial(body, mesh.shape["hid"], mesh.shape["vocab"]),
        mesh=mesh,
        in_specs=(P(None, "vocab", "hid"), P("hid", "vocab"), P(None, "hid")),
        out_specs=(P(None, "hid"), P(None, "hid")),
        check_vma=False,
    )
```
